32 devices in a mesh: prow: 8 (over y, x, core), pcol: 4 (over z).
Axes of the slice: x: 2, y: 2, z: 4, core: 2. Of those that a mesh axis runs over, the one named last changes fastest.
Arguments:
- rhs: bfloat16 [128, 64, 256], P('prow'), may hold values from -6 to 6
- blocks: bfloat16 [128, 16, 256, 256], P('prow', 'pcol'), may hold values from -0.0625 to 0.0625
- inverses: bfloat16 [128, 256, 256], P('prow'), may hold values from -1 to 2.1, as said below
- columns: int32 [128, 16], P('prow', 'pcol'), may hold values from 0 to 127, as said below
- counts: int32 [128, 4], P('prow', 'pcol'), may hold values from 0 to 4, as said below
Outputs:
- solved: bfloat16 [128, 64, 256], P('prow')
The draws below stay inside these ranges and needn't reach their ends.
Inputs may be any that keep to these rules, and one draw needn't show every extreme that they name: `columns`: slot c of array row o names a block row k (level order) of an earlier level than that of o, with (k // 8) % 4 == c // 4, or 0 where no such block row exists; only the first counts[o, c // 4] slots of a group are used. `counts`: 0 where the group has no earlier block row (level 0 in particular); otherwise 1 or more. `inverses`: each tile is the inverse of a lower triangular diagonal block, itself lower triangular.
All inputs are finite; a program needn't handle non-finite values.
Results may differ from the reference program's by a relative error of at most 0.0054.
Values may be sent and summed in bfloat16 or wider, within the bound.
No kernel may reach another device: no remote copies, remote signals or barrier semaphores. Data moves between devices by JAX's collectives and lax.ppermute only.
A program may use at most 64 MiB of HBM per device.

```python
import math
import jax
import jax.numpy as jnp

NB = 256
RHS = 64
LEVELS = 8
LR = 2
KDEV = 4
ROWS_DEV = 16
NBLK = 128
N_PROW = 8
N_PCOL = 4


def group_options(rows, groups):
    level_no = rows % ROWS_DEV // LR
    limit = level_no * LR
    return jnp.maximum((limit - groups + N_PCOL - 1) // N_PCOL, 0)


def draw_inverses(key, part):
    base = jax.random.normal(key, (NBLK, NB, NB), jnp.float32)
    lower = jnp.tril(base, -1) * (0.4 / math.sqrt(NB / 2.0))
    diagonal = jnp.ones((NBLK, NB), jnp.float32)
    eye = jnp.eye(NB, dtype=jnp.float32)
    return (lower + diagonal[:, :, None] * eye[None]).astype(jnp.bfloat16)


def draw_columns(key, part):
    rows = jnp.arange(NBLK, dtype=jnp.int32)[:, None]
    slot_ids = jnp.arange(N_PCOL * KDEV, dtype=jnp.int32)[None, :]
    groups = slot_ids // KDEV
    options = group_options(rows, groups)
    shape = (NBLK, N_PCOL * KDEV)
    picked = jax.random.randint(jax.random.fold_in(key, 11), shape, 0, 1 << 20) % jnp.maximum(options, 1)
    offset = jax.random.randint(jax.random.fold_in(key, 13), shape, 0, N_PROW)
    chosen = (groups + N_PCOL * picked) * N_PROW + offset
    return jnp.where(options > 0, chosen, 0).astype(jnp.int32)


def draw_counts(key, part):
    rows = jnp.arange(NBLK, dtype=jnp.int32)[:, None]
    groups = jnp.arange(N_PCOL, dtype=jnp.int32)[None, :]
    options = group_options(rows, groups)
    drawn = jax.random.randint(jax.random.fold_in(key, 17), (NBLK, N_PCOL), 1, KDEV + 1)
    drawn = jnp.where(options > 0, drawn, 0)
    forced = (rows % ROWS_DEV == LR) & (groups == 0)
    return jnp.where(forced, KDEV, drawn).astype(jnp.int32)


def steps_of(key, shape, cuts, least, largest):
    level = 1.0
    for position, shards_of in cuts:
        draws = jax.random.uniform(jax.random.fold_in(jax.random.fold_in(key, 6), position), (shards_of,), jnp.float32, least / len(cuts), largest / len(cuts))
        level = level * jnp.repeat(jnp.exp(draws), shape[position] // shards_of).reshape((-1,) + (1,) * (len(shape) - 1 - position))
    return level


def bell_draw(key, shape, scale, most, shards=(), kind=jnp.bfloat16):
    values = scale * jax.random.normal(key, shape, jnp.float32)
    if shards:
        values = values * steps_of(key, shape, shards, -0.22, 0.18)
    return jnp.clip(values, -most, most).astype(kind)


def setup_inputs(seed: int = 0) -> dict:
    streams_of = jax.random.split(jax.random.key(seed), 6)
    return {
        "rhs": bell_draw(streams_of[0], (NBLK, RHS, NB), 1.0, 6.0, ((0, 8),)),
        "blocks": bell_draw(streams_of[1], (NBLK, N_PCOL * KDEV, NB, NB), (2 * NB * N_PCOL * KDEV) ** -0.5, 0.0625, ((0, 8), (1, 4))),
        "inverses": draw_inverses(jax.random.fold_in(streams_of[5], 71), 0),
        "columns": draw_columns(jax.random.fold_in(streams_of[5], 71), 0),
        "counts": draw_counts(jax.random.fold_in(streams_of[5], 71), 0),
    }


def level_rows(source, level_no):
    shaped = source.reshape((N_PROW, ROWS_DEV) + source.shape[1:])
    chosen = shaped[:, level_no * LR:(level_no + 1) * LR]
    chosen = jnp.swapaxes(chosen, 0, 1)
    return chosen.reshape((LR * N_PROW,) + source.shape[1:])


def reference(rhs, blocks, inverses, columns, counts):
    per_level = LR * N_PROW
    slot_index = jnp.arange(N_PCOL * KDEV, dtype=jnp.int32)
    live = (slot_index[None, :] % KDEV) < jnp.repeat(counts, KDEV, axis=1)
    solution = jnp.zeros((NBLK, RHS, NB), jnp.bfloat16)
    for level_no in range(LEVELS):
        column_ids = level_rows(columns, level_no)
        active = level_rows(live, level_no)
        gathered = solution[column_ids]
        gathered = jnp.where(active[:, :, None, None], gathered, jnp.zeros_like(gathered))
        panels = level_rows(blocks, level_no).astype(jnp.float32)
        update_sum = jnp.einsum('pcrj,pcij->pri', gathered.astype(jnp.float32), panels)
        right_side = level_rows(rhs, level_no).astype(jnp.float32)
        residual = (right_side - update_sum).astype(jnp.bfloat16)
        inverse_tiles = level_rows(inverses, level_no).astype(jnp.float32)
        solved_now = jnp.einsum('prb,pab->pra', residual.astype(jnp.float32), inverse_tiles)
        solution = solution.at[level_no * per_level:(level_no + 1) * per_level].set(solved_now.astype(jnp.bfloat16))
    shaped = solution.reshape((LEVELS, LR, N_PROW, RHS, NB))
    shaped = jnp.moveaxis(shaped, 2, 0)
    return shaped.reshape((NBLK, RHS, NB))
```

```python
import functools

import jax
import jax.numpy as jnp
from jax import lax
from jax.experimental import pallas as pl
from jax.experimental.pallas import tpu as pltpu
from jax.sharding import PartitionSpec as P

LEVELS = 8
LR = 2
BF16 = jnp.bfloat16
F32 = jnp.float32
VM = pl.BlockSpec(memory_space=pltpu.VMEM)
SM = pl.BlockSpec(memory_space=pltpu.SMEM)


def dot_t(left, right):
    return lax.dot_general(left, right, (((1,), (1,)), ((), ())), preferred_element_type=F32)


def role(level):
    return lax.rem(lax.axis_index("pcol") + 2 * LEVELS * LR * lax.axis_size("pcol") - level * LR, lax.axis_size("pcol"))


def call(body, outs, ins, specs=None, aliases=None):
    return pl.pallas_call(
        body,
        out_shape=outs,
        in_specs=specs or [VM] * len(ins),
        out_specs=[VM] * len(outs),
        input_output_aliases=aliases or {},
    )(*ins)


def spread(store, pieces, level, local):
    rows = 2 * len(pieces)

    def body(*refs):
        out = refs[-1]
        out[...] = refs[0][...]

        @pl.when(role(level) < LR)
        def _():
            for j, piece in enumerate(refs[1:-1]):
                out[pl.ds(local * rows + 2 * j, 2)] = piece[...]

    return call(body, [jax.ShapeDtypeStruct(store.shape, store.dtype)], [store, *pieces])[0]


def partials(level, newest, table, store, own, other, kinds):
    slots = own.shape[1]
    shape = (2, store.shape[1], store.shape[2])

    def row_sum(table_ref, store_ref, own_ref, other_ref, row, pair):
        blocks_ref = other_ref if pair else own_ref
        total = None
        for j in range(slots):
            at = table_ref[level * LR + row, pair * slots + j]
            part = dot_t(store_ref[at], blocks_ref[row, j])
            total = part if total is None else total + part
        return total

    def body(table_ref, store_ref, own_ref, other_ref, *outs):
        place = role(newest) if newest is not None else 0

        def work():
            for out, (turn, kind) in zip(outs, kinds):
                row = lax.rem(place + turn, LR) if newest is not None else turn
                for pair in range(2):
                    out[pair] = row_sum(table_ref, store_ref, own_ref, other_ref, row, pair).astype(kind)

        if newest is None:
            work()
        else:
            pl.when(place < LR)(work)

    outs = [jax.ShapeDtypeStruct(shape, kind) for _, kind in kinds]
    return call(body, outs, [table, store, own, other], specs=[SM, VM, VM, VM])


def solve(level, rhs_own, rhs_other, inv_own, inv_other, terms):
    def body(ro, rp, io, ip, *refs):
        *terms_refs, out = refs
        place = role(level)

        @pl.when(place < LR)
        def _():
            for pair in range(2):
                r_ref, i_ref = (rp, ip) if pair else (ro, io)
                rest = r_ref[place].astype(F32)
                for term in terms_refs:
                    rest = rest - term[pair].astype(F32)
                out[pair] = dot_t(rest.astype(BF16), i_ref[place]).astype(BF16)

    shape = jax.ShapeDtypeStruct((2,) + rhs_own.shape[1:], BF16)
    return call(body, [shape], [rhs_own, rhs_other, inv_own, inv_other, *terms])[0]


def solve_first(rhs, inv, half):
    def body(r, i, keep, send):
        place = role(0)
        core = lax.rem(lax.axis_index("prow"), 2)

        @pl.when(place < LR)
        def _():
            tile = i[place]
            for out, part in ((keep, core), (send, 1 - core)):
                out[...] = dot_t(r[place, pl.ds(pl.multiple_of(part * half, half), half)], tile).astype(BF16)

    shape = jax.ShapeDtypeStruct((half, rhs.shape[2]), BF16)
    return call(body, [shape, shape], [rhs, inv])


def solve_last(rhs_own, rhs_other, inv_own, inv_other, parts):
    count = len(parts)

    def body(ro, rp, io, ip, *refs):
        own, other, held = refs[-3:]
        me = lax.axis_index("pcol")
        for k in range(count):
            held[jnp.bitwise_xor(me, k)] = refs[k][...]
        for pair in range(2):
            r_ref, i_ref, out = (rp, ip, other) if pair else (ro, io, own)
            for row in range(LR):
                rest = r_ref[row].astype(F32)
                for k in range(count):
                    rest = rest - held[k, row, pair].astype(F32)
                out[row] = dot_t(rest.astype(BF16), i_ref[row]).astype(BF16)

    shape = jax.ShapeDtypeStruct(rhs_own.shape, BF16)
    return pl.pallas_call(
        body,
        out_shape=[shape, shape],
        in_specs=[VM] * (4 + count),
        out_specs=[VM, VM],
        scratch_shapes=[pltpu.VMEM((count,) + parts[0].shape, BF16)],
    )(rhs_own, rhs_other, inv_own, inv_other, *parts)


def body(rhs, blocks, inverses, columns, counts):
    rows, sides, size = rhs.shape
    slots = columns.shape[1]
    half = sides // 2
    prow_count = lax.axis_size("prow")
    pcol_count = lax.axis_size("pcol")
    groups = pcol_count // LR
    locals_count = rows // pcol_count
    me = lax.axis_index("prow")
    core = me % 2

    def prow_swap(x, k):
        return lax.ppermute(x, "prow", [(i, i ^ k) for i in range(prow_count)])

    def pcol_swap(x, k):
        return lax.ppermute(x, "pcol", [(i, i ^ k) for i in range(pcol_count)])

    def between(x, first, second, turn):
        pairs = []
        for a in range(LR):
            s, d = (first * LR + a) % pcol_count, (second * LR + (a + turn) % LR) % pcol_count
            pairs += [(s, d), (d, s)]
        return lax.ppermute(x, "pcol", sorted(set(pairs)))

    keep, send = solve_first(rhs[:LR], inverses[:LR], half)
    solved = [jnp.stack([keep, prow_swap(send, 1)])]

    live = jnp.arange(slots, dtype=jnp.int32)[None, :] < counts
    coded = jnp.where(live, columns, -1)
    coded = jnp.concatenate([coded, prow_swap(coded, 1)], axis=1)
    zero_row = locals_count * prow_count
    at = coded // prow_count // pcol_count * prow_count + ((coded % prow_count) ^ me)
    table = jnp.where(coded < 0, zero_row, at)
    halves = rhs.reshape(rows, 2, half, size)
    mine = lax.dynamic_index_in_dim(halves, core, 1, keepdims=False)
    theirs = prow_swap(lax.dynamic_index_in_dim(halves, 1 - core, 1, keepdims=False), 1)
    near = prow_swap(blocks[LR:2 * LR], 1)
    far = prow_swap(blocks, 1)
    inverses_other = prow_swap(inverses, 1)

    def own_blocks(level):
        return blocks[level * LR:(level + 1) * LR]

    def other_blocks(level):
        return near if level == 1 else far[level * LR:(level + 1) * LR]

    def level_of(x, level):
        return x[level * LR:(level + 1) * LR]

    store = jnp.zeros((zero_row + 1, half, size), BF16)
    waiting = {level: [] for level in range(LEVELS)}
    for level in range(1, LEVELS):
        newest = level - 1
        y = solved[newest]
        pieces = [y] + [prow_swap(y, k) for k in range(2, prow_count, 2)]
        store = spread(store, pieces, newest, newest * LR // pcol_count)
        if level == LEVELS - 1:
            parts = partials(level, None, table, store, own_blocks(level), other_blocks(level), [(0, BF16), (1, BF16)])
            whole = jnp.stack(parts)
            final = [whole] + [pcol_swap(whole, k) for k in range(1, pcol_count)]
            own, other = solve_last(level_of(mine, level), level_of(theirs, level), level_of(inverses, level),
                                    level_of(inverses_other, level), final)
            break
        straight, crossed = partials(level, newest, table, store, own_blocks(level), other_blocks(level), [(0, BF16), (1, BF16)])
        terms = [between(straight, newest, level, 0), between(crossed, newest, level, 1)]
        for ahead in range(1, groups):
            later = level + ahead
            if later >= LEVELS - 1:
                continue
            mine_next = ahead == groups - 1
            kinds = [(0, F32 if mine_next else BF16), (1, BF16)]
            a, b = partials(later, newest, table, store, own_blocks(later), other_blocks(later), kinds)
            if mine_next:
                waiting[later] += [a, between(b, newest, newest, 1)]
            else:
                waiting[later] += [between(a, newest, later, 0), between(b, newest, later, 1)]
        solved.append(solve(level, level_of(mine, level), level_of(theirs, level), level_of(inverses, level),
                            level_of(inverses_other, level), terms + waiting[level]))

    group = lax.axis_index("pcol") // LR
    done = LEVELS - 1
    cycles = -(-done // groups)
    held = []
    for i in range(cycles):
        pick = solved[min(i * groups, done - 1)]
        for g in range(1, groups):
            pick = jnp.where(group == g, solved[min(i * groups + g, done - 1)], pick)
        held.append(pick)
    held = jnp.stack(held)
    held = jnp.stack([held[:, 0], prow_swap(held[:, 1], 1)], axis=1)
    spread_rows = [held] + [pcol_swap(held, k) for k in range(1, pcol_count)]
    swapped = prow_swap(other, 1)

    def assemble(*refs):
        *sources, own_ref, swapped_ref, out = refs
        col = lax.axis_index("pcol")
        my_core = lax.rem(lax.axis_index("prow"), 2)
        mine_at = pl.ds(pl.multiple_of(my_core * half, half), half)
        theirs_at = pl.ds(pl.multiple_of((1 - my_core) * half, half), half)
        for k, source in enumerate(sources):
            for i in range(cycles):
                row = i * pcol_count + jnp.bitwise_xor(col, k)
                out[row, mine_at] = source[i, 0]
                out[row, theirs_at] = source[i, 1]
        for s in range(LR):
            out[done * LR + s, mine_at] = own_ref[s]
            out[done * LR + s, theirs_at] = swapped_ref[s]

    return call(assemble, [jax.ShapeDtypeStruct(rhs.shape, BF16)], [*spread_rows, own, swapped])[0]


def solution(mesh):
    placed = (
        P("prow", None, None),
        P("prow", "pcol", None, None),
        P("prow", None, None),
        P("prow", "pcol"),
        P("prow", "pcol"),
    )
    return jax.shard_map(
        body, mesh=mesh, in_specs=placed, out_specs=P("prow", None, None), check_vma=False
    )
```

```python
import jax
import jax.numpy as jnp
from jax import lax
from jax.experimental import pallas as pl
from jax.experimental.pallas import tpu as pltpu
from jax.sharding import PartitionSpec as P


LEVELS = 8
LR = 2
BF16 = jnp.bfloat16
F32 = jnp.float32
LIMIT = 4 << 20
VM = pl.BlockSpec(memory_space=pltpu.VMEM)
HBM = pl.BlockSpec(memory_space=pltpu.HBM)
SM = pl.BlockSpec(memory_space=pltpu.SMEM)


def dot_t(left, right):
    return lax.dot_general(left, right, (((1,), (1,)), ((), ())), preferred_element_type=F32)


def role(level):
    return lax.rem(lax.axis_index("pcol") + 2 * LEVELS * LR * lax.axis_size("pcol") - level * LR, lax.axis_size("pcol"))


def call(body, outs, ins, specs=None, aliases=None, scratch=(), limit=LIMIT):
    specs = specs or [VM] * len(ins)
    ins = [pltpu.with_memory_space_constraint(x, spec.memory_space) for x, spec in zip(ins, specs)]
    return pl.pallas_call(
        body,
        out_shape=[pltpu.VMEM(shape, kind) for shape, kind in outs],
        in_specs=specs,
        out_specs=[VM] * len(outs),
        input_output_aliases=aliases or {},
        scratch_shapes=scratch,
        compiler_params=pltpu.CompilerParams(vmem_limit_bytes=limit),
    )(*ins)


def row_sum(table, store, own, other, level, row, pair):
    slots = own.shape[1] - 1
    total = None
    for j in range(slots):
        at = table[level * LR + row, pair * slots + j]
        part = dot_t(store[at], (other if pair else own)[row, j])
        total = part if total is None else total + part
    return total


def update(level, table, store, pieces, own, other):
    newest = level - 1
    last = level == LEVELS - 1
    base = newest * LR // lax.axis_size("pcol") * 2 * len(pieces)

    def body(table_ref, store_ref, own_ref, other_ref, *refs):
        pieces_refs, out, sums = refs[:len(pieces)], refs[len(pieces)], refs[len(pieces) + 1:]
        place = role(newest)

        @pl.when(place < LR)
        def _():
            for j, piece in enumerate(pieces_refs):
                out[pl.ds(base + 2 * j, 2)] = piece[...]
            if not last:
                add_rows(level, place, table_ref, out, own_ref, other_ref, sums)

        if last:
            add_rows(level, place, table_ref, out, own_ref, other_ref, sums)
        else:
            @pl.when(place >= LR)
            def _():
                for to in sums:
                    to[...] = pieces_refs[0][...]

    shape = (2,) + store.shape[1:]
    sums = [((LR,) + shape, BF16)] if last else [(shape, BF16), (shape, BF16)]
    return call(body, [(store.shape, BF16), *sums], [table, store, own, other, *pieces],
                specs=[SM] + [VM] * (3 + len(pieces)), aliases={1: 0})


def add_rows(level, place, table, store, own, other, sums):
    for turn in range(LR):
        row = turn if len(sums) == 1 else lax.rem(place + turn, LR)
        for pair in range(2):
            total = row_sum(table, store, own, other, level, row, pair)
            if len(sums) == 1:
                sums[0][turn, pair] = total.astype(BF16)
            else:
                sums[turn][pair] = total.astype(sums[turn].dtype)


def early(level, newest, table, store, own, other, kind, solved):
    def body(table_ref, store_ref, own_ref, other_ref, solved_ref, *sums):
        place = role(newest)

        @pl.when(place < LR)
        def _():
            add_rows(level, place, table_ref, store_ref, own_ref, other_ref, sums)

        @pl.when(place >= LR)
        def _():
            sums[1][...] = solved_ref[...]

    shape = (2,) + store.shape[1:]
    return call(body, [(shape, kind), (shape, BF16)], [table, store, own, other, solved], specs=[SM, VM, VM, VM, VM])


def solve(level, rhs_own, rhs_other, own, other, before, terms):
    def body(ro, rp, io, ip, old, *refs):
        *terms_refs, out = refs
        place = role(level)

        @pl.when(place < LR)
        def _():
            for pair in range(2):
                r_ref, i_ref = (rp, ip) if pair else (ro, io)
                rest = r_ref[level * LR + place].astype(F32)
                for term in terms_refs:
                    rest = rest - term[pair].astype(F32)
                out[pair] = dot_t(rest.astype(BF16), i_ref[place, i_ref.shape[1] - 1]).astype(BF16)

        @pl.when(place >= LR)
        def _():
            out[...] = old[...]

    return call(body, [(before.shape, BF16)], [rhs_own, rhs_other, own, other, before, *terms])[0]


def solve_first(rhs, inverses, half):
    def body(r, i, keep, send, side, tile, sems):
        place = role(0)
        core = lax.rem(lax.axis_index("prow"), 2)
        at = lax.rem(place, LR)
        copies = [pltpu.make_async_copy(r.at[at], side, sems.at[0]), pltpu.make_async_copy(i.at[at], tile, sems.at[1])]
        for copy in copies:
            copy.start()
        for copy in copies:
            copy.wait()
        for out, part in ((keep, core), (send, 1 - core)):
            out[...] = dot_t(side[pl.ds(pl.multiple_of(part * half, half), half)], tile[...]).astype(BF16)

    size = rhs.shape[2]
    shape = ((half, size), BF16)
    return call(body, [shape, shape], [rhs, inverses], specs=[HBM] * 2,
                scratch=[pltpu.VMEM(rhs.shape[1:], BF16), pltpu.VMEM((size, size), BF16), pltpu.SemaphoreType.DMA((2,))])


def join(a, b):
    def body(x, y, out):
        out[0] = x[...]
        out[1] = y[...]

    return call(body, [((2,) + a.shape, BF16)], [a, b])[0]


def stage(level, inverses, blocks, after=()):
    slots = blocks.shape[1]
    rows = pl.ds(level * LR, LR)

    def body(i, b, *refs):
        out, sems = refs[-2:]
        copies = [pltpu.make_async_copy(b.at[rows], out.at[:, pl.ds(0, slots)], sems.at[0]),
                  pltpu.make_async_copy(i.at[rows], out.at[:, slots], sems.at[1])]
        for copy in copies:
            copy.start()
        for copy in copies:
            copy.wait()

    return call(body, [((LR, slots + 1) + blocks.shape[2:], BF16)], [inverses, blocks, *after],
                specs=[HBM] * 2 + [VM] * len(after), scratch=[pltpu.SemaphoreType.DMA((2,))])[0]


def halves(rhs, half):
    def body(r, mine, give, sems):
        core = lax.rem(lax.axis_index("prow"), 2)
        copies = []
        for k, (out, part) in enumerate(((mine, core), (give, 1 - core))):
            copies.append(pltpu.make_async_copy(r.at[:, pl.ds(pl.multiple_of(part * half, half), half)], out, sems.at[k]))
        for copy in copies:
            copy.start()
        for copy in copies:
            copy.wait()

    shape = ((rhs.shape[0], half, rhs.shape[2]), BF16)
    return call(body, [shape, shape], [rhs], specs=[HBM], scratch=[pltpu.SemaphoreType.DMA((2,))])


def zeros(shape):
    def body(out):
        out[...] = jnp.zeros(shape, BF16)

    return call(body, [(shape, BF16)], [])[0]


def to_scalars(table):
    def body(x, out):
        for i in range(table.shape[0]):
            for j in range(table.shape[1]):
                out[i, j] = x[i, j]

    return pl.pallas_call(body, out_shape=pltpu.SMEM(table.shape, jnp.int32), in_specs=[SM], out_specs=SM)(table)


def place_rows(found, col, write):
    for level, ref, away in found:
        source = jnp.bitwise_xor(col, away)
        count = lax.axis_size("pcol")
        place = lax.rem(source + 2 * LEVELS * LR * count - level * LR, count)

        @pl.when(place < LR)
        def _():
            write(level * LR + place, ref)


def pack(found, levels, half, size):
    first = levels[0] * LR

    def body(*refs):
        *sources, out = refs

        def write(row, ref):
            out[row - first] = ref[1]

        place_rows([(level, ref, away) for (level, _, away), ref in zip(found, sources)], lax.axis_index("pcol"), write)

    return call(body, [((len(levels) * LR, half, size), BF16)], [x for _, x, _ in found])[0]


def solve_last(rhs_own, rhs_other, own_tiles, other_tiles, parts, found, first):
    count = len(parts)
    half, size = rhs_own.shape[1:]

    def body(ro, rp, io, ip, *refs):
        parts_refs, sources, (own, send, held) = refs[:count], refs[count:-3], refs[-3:]
        col = lax.axis_index("pcol")
        for k in range(count):
            held[jnp.bitwise_xor(col, k)] = parts_refs[k][...]
        for pair in range(2):
            r_ref, i_ref = (rp, ip) if pair else (ro, io)
            for row in range(LR):
                rest = r_ref[(LEVELS - 1) * LR + row].astype(F32)
                for k in range(count):
                    rest = rest - held[k, row, pair].astype(F32)
                done = dot_t(rest.astype(BF16), i_ref[row, i_ref.shape[1] - 1]).astype(BF16)
                if pair:
                    send[(LEVELS - 1 - first) * LR + row] = done
                else:
                    own[row] = done

        def write(row, ref):
            send[row - first * LR] = ref[1]

        place_rows([(level, ref, away) for (level, _, away), ref in zip(found, sources)], col, write)

    outs = [((LR, half, size), BF16), (((LEVELS - first) * LR, half, size), BF16)]
    return call(body, outs, [rhs_own, rhs_other, own_tiles, other_tiles, *parts, *[x for _, x, _ in found]],
                scratch=[pltpu.VMEM((count,) + parts[0].shape, BF16)])


def assemble(found, swapped, own, shape):
    half = shape[1] // 2

    def body(*refs):
        sources, swaps, own_ref, out = refs[:len(found)], refs[len(found):-2], refs[-2], refs[-1]
        col = lax.axis_index("pcol")
        core = lax.rem(lax.axis_index("prow"), 2)
        mine_at = pl.ds(pl.multiple_of(core * half, half), half)
        theirs_at = pl.ds(pl.multiple_of((1 - core) * half, half), half)

        def write(row, ref):
            out[row, mine_at] = ref[0]

        place_rows([(level, ref, away) for (level, _, away), ref in zip(found, sources)], col, write)
        row = 0
        for ref in swaps:
            for i in range(ref.shape[0]):
                out[row, theirs_at] = ref[i]
                row += 1
        for i in range(LR):
            out[(LEVELS - 1) * LR + i, mine_at] = own_ref[i]

    return call(body, [(shape, BF16)], [*[x for _, x, _ in found], *swapped, own])[0]


def body(rhs, blocks, inverses, columns, counts):
    rows, sides, size = rhs.shape
    slots = columns.shape[1]
    half = sides // 2
    prow_count = lax.axis_size("prow")
    pcol_count = lax.axis_size("pcol")
    groups = pcol_count // LR
    paired = groups == 2
    me = lax.axis_index("prow")

    def prow_swap(x, k):
        return lax.ppermute(x, "prow", [(i, i ^ k) for i in range(prow_count)])

    def pcol_swap(x, k):
        return lax.ppermute(x, "pcol", [(i, i ^ k) for i in range(pcol_count)])

    def between(x, first, second, turn):
        pairs = []
        for a in range(LR):
            s, d = (first * LR + a) % pcol_count, (second * LR + (a + turn) % LR) % pcol_count
            pairs += [(s, d), (d, s)]
        return lax.ppermute(x, "pcol", sorted(set(pairs)))

    def share(x):
        return [x] + [pcol_swap(x, k) for k in range(1, pcol_count)]

    keep, send = solve_first(rhs, inverses, half)
    solved = [join(keep, prow_swap(send, 1))]
    held = {1: stage(1, inverses, blocks)}
    other = {1: prow_swap(held[1], 1)}
    live = jnp.arange(slots, dtype=jnp.int32)[None, :] < counts
    coded = jnp.where(live, columns, -1)
    coded = jnp.concatenate([coded, prow_swap(coded, 1)], axis=1)
    zero_row = rows // pcol_count * prow_count
    at = coded // prow_count // pcol_count * prow_count + ((coded % prow_count) ^ me)
    table = to_scalars(jnp.where(coded < 0, zero_row, at))
    mine, give = halves(rhs, half)
    theirs = prow_swap(give, 1)

    store = zeros((zero_row + 1, half, size))
    waiting = {level: [] for level in range(LEVELS)}
    found = []
    for level in range(1, LEVELS):
        newest = level - 1
        last = level == LEVELS - 1
        y = solved[newest]
        pieces = [y] + [prow_swap(y, k) for k in range(2, prow_count, 2)]
        if last:
            late = [newest - g for g in range(groups)] if paired else list(range(newest, -1, -1))
            rest = [(late[:groups], y)] if paired else [([i], solved[i]) for i in late]
            spread = [(y, share(y))] if paired else [(solved[i], share(solved[i])) for i in late]
            for (levels, _), (_, copies) in zip(rest, spread):
                found += [(i, copy, k) for i in levels for k, copy in enumerate(copies)]
        store, *sums = update(level, table, store, pieces, held[level], other[level])
        if last:
            parts = share(sums[0])
            break
        terms = [between(sums[0], newest, level, 0)]
        terms.append(between(sums[1], newest, level, 1))
        reach = level + groups
        for later in [reach] if level > 1 else range(2, reach + 1):
            if later < LEVELS:
                held[later] = stage(later, inverses, blocks, sums)
                other[later] = prow_swap(held[later], 1)
        traded = None
        for ahead in range(1, groups):
            later = level + ahead
            if later >= LEVELS - 1:
                continue
            own_pair = ahead == groups - 1
            a, b = early(later, newest, table, store, held[later], other[later], F32 if own_pair else BF16, y)
            if paired:
                traded = pcol_swap(b, 1)
                waiting[later] += [a, traded]
            elif own_pair:
                waiting[later] += [a, between(b, newest, newest, 1)]
            else:
                waiting[later] += [between(a, newest, later, 0), between(b, newest, later, 1)]
        if paired and level > 1:
            if traded is None:
                traded = pcol_swap(y, 1)
            found += [(level - 2, y, 0), (level - 2, traded, 1)]
            found += [(level - 2, terms[0], 2), (level - 2, terms[1], 3)]
        solved.append(solve(level, mine, theirs, held[level], other[level], y, terms + waiting[level]))

    first = min(late)
    swapped = [prow_swap(pack([f for f in found if f[0] < first], list(range(first)), half, size), 1)] if first else []
    own, send = solve_last(mine, theirs, held[LEVELS - 1], other[LEVELS - 1], parts,
                           [f for f in found if f[0] >= first], first)
    return assemble(found, swapped + [prow_swap(send, 1)], own, rhs.shape)


def solution(mesh):
    placed = (
        P("prow", None, None),
        P("prow", "pcol", None, None),
        P("prow", None, None),
        P("prow", "pcol"),
        P("prow", "pcol"),
    )
    return jax.shard_map(
        body, mesh=mesh, in_specs=placed, out_specs=P("prow", None, None), check_vma=False
    )
```

```python
import jax
import jax.numpy as jnp
from jax import lax
from jax.experimental import pallas as pl
from jax.experimental.pallas import tpu as pltpu
from jax.sharding import PartitionSpec as P


LEVELS = 8
LR = 2
BF16 = jnp.bfloat16
F32 = jnp.float32
LIMIT = 4 << 20
VM = pl.BlockSpec(memory_space=pltpu.VMEM)
HBM = pl.BlockSpec(memory_space=pltpu.HBM)
SM = pl.BlockSpec(memory_space=pltpu.SMEM)


def dot_t(left, right):
    return lax.dot_general(left, right, (((1,), (1,)), ((), ())), preferred_element_type=F32)


def role(level):
    return lax.rem(lax.axis_index("pcol") + 2 * LEVELS * LR * lax.axis_size("pcol") - level * LR, lax.axis_size("pcol"))


def call(body, outs, ins, specs=None, aliases=None, scratch=(), limit=LIMIT):
    specs = specs or [VM] * len(ins)
    ins = [pltpu.with_memory_space_constraint(x, spec.memory_space) for x, spec in zip(ins, specs)]
    return pl.pallas_call(
        body,
        out_shape=[pltpu.VMEM(shape, kind) for shape, kind in outs],
        in_specs=specs,
        out_specs=[VM] * len(outs),
        input_output_aliases=aliases or {},
        scratch_shapes=scratch,
        compiler_params=pltpu.CompilerParams(vmem_limit_bytes=limit),
    )(*ins)


def row_sum(table, store, own, other, level, row, pair):
    slots = own.shape[1] - 1
    total = None
    for j in range(slots):
        at = table[level * LR + row, pair * slots + j]
        part = dot_t(store[at], (other if pair else own)[row, j])
        total = part if total is None else total + part
    return total


def update(level, table, store, pieces, own, other):
    newest = level - 1
    last = level == LEVELS - 1
    base = newest * LR // lax.axis_size("pcol") * 2 * len(pieces)

    def body(table_ref, store_ref, own_ref, other_ref, *refs):
        pieces_refs, out, sums = refs[:len(pieces)], refs[len(pieces)], refs[len(pieces) + 1:]
        place = role(newest)

        @pl.when(place < LR)
        def _():
            for j, piece in enumerate(pieces_refs):
                out[pl.ds(base + 2 * j, 2)] = piece[...]
            if not last:
                add_rows(level, place, table_ref, out, own_ref, other_ref, sums)

        if last:
            add_rows(level, place, table_ref, out, own_ref, other_ref, sums)
        else:
            @pl.when(place >= LR)
            def _():
                for to in sums:
                    to[...] = pieces_refs[0][...]

    shape = (2,) + store.shape[1:]
    sums = [((LR,) + shape, BF16)] if last else [(shape, BF16), (shape, BF16)]
    return call(body, [(store.shape, BF16), *sums], [table, store, own, other, *pieces],
                specs=[SM] + [VM] * (3 + len(pieces)), aliases={1: 0})


def add_rows(level, place, table, store, own, other, sums):
    for turn in range(LR):
        row = turn if len(sums) == 1 else lax.rem(place + turn, LR)
        for pair in range(2):
            total = row_sum(table, store, own, other, level, row, pair)
            if len(sums) == 1:
                sums[0][turn, pair] = total.astype(BF16)
            else:
                sums[turn][pair] = total.astype(sums[turn].dtype)


def early(level, newest, table, store, own, other, kind, solved):
    def body(table_ref, store_ref, own_ref, other_ref, solved_ref, *sums):
        place = role(newest)

        @pl.when(place < LR)
        def _():
            add_rows(level, place, table_ref, store_ref, own_ref, other_ref, sums)

        @pl.when(place >= LR)
        def _():
            sums[1][...] = solved_ref[...]

    shape = (2,) + store.shape[1:]
    return call(body, [(shape, kind), (shape, BF16)], [table, store, own, other, solved], specs=[SM, VM, VM, VM, VM])


def solve(level, rhs_own, rhs_other, own, other, before, terms):
    def body(ro, rp, io, ip, old, *refs):
        *terms_refs, out = refs
        place = role(level)

        @pl.when(place < LR)
        def _():
            for pair in range(2):
                r_ref, i_ref = (rp, ip) if pair else (ro, io)
                rest = r_ref[level * LR + place].astype(F32)
                for term in terms_refs:
                    rest = rest - term[pair].astype(F32)
                out[pair] = dot_t(rest.astype(BF16), i_ref[place, i_ref.shape[1] - 1]).astype(BF16)

        @pl.when(place >= LR)
        def _():
            out[...] = old[...]

    return call(body, [(before.shape, BF16)], [rhs_own, rhs_other, own, other, before, *terms])[0]


def solve_first(rhs, inverses, half):
    def body(r, i, keep, send, side, tile, sems):
        place = role(0)
        core = lax.rem(lax.axis_index("prow"), 2)
        at = lax.rem(place, LR)
        copies = [pltpu.make_async_copy(r.at[at], side, sems.at[0]), pltpu.make_async_copy(i.at[at], tile, sems.at[1])]
        for copy in copies:
            copy.start()
        for copy in copies:
            copy.wait()
        for out, part in ((keep, core), (send, 1 - core)):
            out[...] = dot_t(side[pl.ds(pl.multiple_of(part * half, half), half)], tile[...]).astype(BF16)

    size = rhs.shape[2]
    shape = ((half, size), BF16)
    return call(body, [shape, shape], [rhs, inverses], specs=[HBM] * 2,
                scratch=[pltpu.VMEM(rhs.shape[1:], BF16), pltpu.VMEM((size, size), BF16), pltpu.SemaphoreType.DMA((2,))])


def join(a, b):
    def body(x, y, out):
        out[0] = x[...]
        out[1] = y[...]

    return call(body, [((2,) + a.shape, BF16)], [a, b])[0]


def stage(level, inverses, blocks, after=()):
    slots = blocks.shape[1]
    rows = pl.ds(level * LR, LR)

    def body(i, b, *refs):
        out, sems = refs[-2:]
        copies = [pltpu.make_async_copy(b.at[rows], out.at[:, pl.ds(0, slots)], sems.at[0]),
                  pltpu.make_async_copy(i.at[rows], out.at[:, slots], sems.at[1])]
        for copy in copies:
            copy.start()
        for copy in copies:
            copy.wait()

    return call(body, [((LR, slots + 1) + blocks.shape[2:], BF16)], [inverses, blocks, *after],
                specs=[HBM] * 2 + [VM] * len(after), scratch=[pltpu.SemaphoreType.DMA((2,))])[0]


def halves(rhs, half):
    def body(r, mine, give, sems):
        core = lax.rem(lax.axis_index("prow"), 2)
        copies = []
        for k, (out, part) in enumerate(((mine, core), (give, 1 - core))):
            copies.append(pltpu.make_async_copy(r.at[:, pl.ds(pl.multiple_of(part * half, half), half)], out, sems.at[k]))
        for copy in copies:
            copy.start()
        for copy in copies:
            copy.wait()

    shape = ((rhs.shape[0], half, rhs.shape[2]), BF16)
    return call(body, [shape, shape], [rhs], specs=[HBM], scratch=[pltpu.SemaphoreType.DMA((2,))])


def zeros(shape):
    def body(out):
        out[...] = jnp.zeros(shape, BF16)

    return call(body, [(shape, BF16)], [])[0]


def to_scalars(table):
    def body(x, out):
        for i in range(table.shape[0]):
            for j in range(table.shape[1]):
                out[i, j] = x[i, j]

    return pl.pallas_call(body, out_shape=pltpu.SMEM(table.shape, jnp.int32), in_specs=[SM], out_specs=SM)(table)


def place_rows(found, col, write):
    for level, ref, away in found:
        source = jnp.bitwise_xor(col, away)
        count = lax.axis_size("pcol")
        place = lax.rem(source + 2 * LEVELS * LR * count - level * LR, count)

        @pl.when(place < LR)
        def _():
            write(level * LR + place, ref)


def pack(found, late, first):
    half, size = late[0].shape[1:]

    def body(*refs):
        sources, late_refs, out = refs[:len(found)], refs[len(found):-1], refs[-1]

        def write(row, ref):
            out[row] = ref[1]

        place_rows([(level, ref, away) for (level, _, away), ref in zip(found, sources)], lax.axis_index("pcol"), write)
        for i, ref in enumerate(late_refs):
            out[first * LR + i] = ref[1]

    return call(body, [((first * LR + len(late), half, size), BF16)], [*[x for _, x, _ in found], *late])[0]


def whole_rows(late, swapped, first):
    def body(*refs):
        late_refs, swapped_ref, outs = refs[:len(late)], refs[len(late)], refs[len(late) + 1:]
        for i, (ref, out) in enumerate(zip(late_refs, outs)):
            out[0] = ref[0]
            out[1] = swapped_ref[first * LR + i]

    return call(body, [(y.shape, BF16) for y in late], [*late, swapped])


def solve_last(rhs_own, rhs_other, own_tiles, other_tiles, parts):
    count = len(parts)

    def body(ro, rp, io, ip, *refs):
        *parts_refs, own, send, held = refs
        col = lax.axis_index("pcol")
        for k in range(count):
            held[jnp.bitwise_xor(col, k)] = parts_refs[k][...]
        for r_ref, i_ref, pair, out in ((rp, ip, 1, send), (ro, io, 0, own)):
            for row in range(LR):
                rest = r_ref[(LEVELS - 1) * LR + row].astype(F32)
                for k in range(count):
                    rest = rest - held[k, row, pair].astype(F32)
                out[row] = dot_t(rest.astype(BF16), i_ref[row, i_ref.shape[1] - 1]).astype(BF16)

    shape = ((LR,) + rhs_own.shape[1:], BF16)
    return call(body, [shape, shape], [rhs_own, rhs_other, own_tiles, other_tiles, *parts],
                scratch=[pltpu.VMEM((count,) + parts[0].shape, BF16)])


def assemble(found, late, swapped, own, last_swapped, shape, first):
    half = shape[1] // 2

    def body(*refs):
        sources, (swapped_ref, own_ref, last_ref, out) = refs[:-4], refs[-4:]
        col = lax.axis_index("pcol")
        core = lax.rem(lax.axis_index("prow"), 2)
        mine_at = pl.ds(pl.multiple_of(core * half, half), half)
        theirs_at = pl.ds(pl.multiple_of((1 - core) * half, half), half)

        def write(row, ref):
            out[row, mine_at] = ref[0]

        def write_both(row, ref):
            out[row, mine_at] = ref[0]
            out[row, theirs_at] = ref[1]

        place_rows([(level, ref, away) for (level, _, away), ref in zip(found, sources)], col, write)
        place_rows([(level, ref, away) for (level, _, away), ref in zip(late, sources[len(found):])], col, write_both)
        for row in range(first * LR):
            out[row, theirs_at] = swapped_ref[row]
        for i in range(LR):
            out[(LEVELS - 1) * LR + i, mine_at] = own_ref[i]
            out[(LEVELS - 1) * LR + i, theirs_at] = last_ref[i]

    ins = [*[x for _, x, _ in found + late], swapped, own, last_swapped]
    return call(body, [(shape, BF16)], ins)[0]


def body(rhs, blocks, inverses, columns, counts):
    rows, sides, size = rhs.shape
    slots = columns.shape[1]
    half = sides // 2
    prow_count = lax.axis_size("prow")
    pcol_count = lax.axis_size("pcol")
    groups = pcol_count // LR
    paired = groups == 2
    me = lax.axis_index("prow")

    def prow_swap(x, k):
        return lax.ppermute(x, "prow", [(i, i ^ k) for i in range(prow_count)])

    def pcol_swap(x, k):
        return lax.ppermute(x, "pcol", [(i, i ^ k) for i in range(pcol_count)])

    def between(x, first, second, turn):
        pairs = []
        for a in range(LR):
            s, d = (first * LR + a) % pcol_count, (second * LR + (a + turn) % LR) % pcol_count
            pairs += [(s, d), (d, s)]
        return lax.ppermute(x, "pcol", sorted(set(pairs)))

    def share(x):
        return [x] + [pcol_swap(x, k) for k in range(1, pcol_count)]

    keep, send = solve_first(rhs, inverses, half)
    solved = [join(keep, prow_swap(send, 1))]
    held = {1: stage(1, inverses, blocks)}
    other = {1: prow_swap(held[1], 1)}
    live = jnp.arange(slots, dtype=jnp.int32)[None, :] < counts
    coded = jnp.where(live, columns, -1)
    coded = jnp.concatenate([coded, prow_swap(coded, 1)], axis=1)
    zero_row = rows // pcol_count * prow_count
    at = coded // prow_count // pcol_count * prow_count + ((coded % prow_count) ^ me)
    table = to_scalars(jnp.where(coded < 0, zero_row, at))
    mine, give = halves(rhs, half)
    theirs = prow_swap(give, 1)

    store = zeros((zero_row + 1, half, size))
    waiting = {level: [] for level in range(LEVELS)}
    found = []
    for level in range(1, LEVELS):
        newest = level - 1
        last = level == LEVELS - 1
        y = solved[newest]
        pieces = [y]
        for k in range(2, prow_count, 2):
            pieces.append(prow_swap(y, k))
        if last:
            late = [([newest - g for g in range(groups)], y)] if paired else [([i], x) for i, x in enumerate(solved)]
            first = min(min(levels) for levels, _ in late)
            swapped = prow_swap(pack(found, [x for _, x in late], first), 1)
        store, *sums = update(level, table, store, pieces, held[level], other[level])
        if last:
            parts = share(sums[0])
            rows_late = whole_rows([x for _, x in late], swapped, first)
            spread = [(i, copy, k) for (levels, _), x in zip(late, rows_late)
                      for k, copy in enumerate(share(x)) for i in levels]
            own, send = solve_last(mine, theirs, held[level], other[level], parts)
            return assemble(found, spread, swapped, own, prow_swap(send, 1), rhs.shape, first)
        terms = [between(sums[0], newest, level, 0)]
        terms.append(between(sums[1], newest, level, 1))
        reach = level + groups
        for later in [reach] if level > 1 else range(2, reach + 1):
            if later < LEVELS:
                held[later] = stage(later, inverses, blocks, sums)
                other[later] = prow_swap(held[later], 1)
        traded = None
        for ahead in range(1, groups):
            later = level + ahead
            if later >= LEVELS - 1:
                continue
            own_pair = ahead == groups - 1
            a, b = early(later, newest, table, store, held[later], other[later], F32 if own_pair else BF16, y)
            if paired:
                traded = pcol_swap(b, 1)
                waiting[later] += [a, traded]
            elif own_pair:
                waiting[later] += [a, between(b, newest, newest, 1)]
            else:
                waiting[later] += [between(a, newest, later, 0), between(b, newest, later, 1)]
        if paired and level > 1:
            if traded is None:
                traded = pcol_swap(y, 1)
            found += [(level - 2, y, 0), (level - 2, traded, 1)]
            found += [(level - 2, terms[0], 2), (level - 2, terms[1], 3)]
        solved.append(solve(level, mine, theirs, held[level], other[level], y, terms + waiting[level]))


def solution(mesh):
    placed = (
        P("prow", None, None),
        P("prow", "pcol", None, None),
        P("prow", None, None),
        P("prow", "pcol"),
        P("prow", "pcol"),
    )
    return jax.shard_map(
        body, mesh=mesh, in_specs=placed, out_specs=P("prow", None, None), check_vma=False
    )
```

```python
import jax
import jax.numpy as jnp
from jax import lax
from jax.experimental import pallas as pl
from jax.experimental.pallas import tpu as pltpu
from jax.sharding import PartitionSpec as P


LEVELS = 8
LR = 2
BF16 = jnp.bfloat16
F32 = jnp.float32
LIMIT = 4 << 20
VM = pl.BlockSpec(memory_space=pltpu.VMEM)
HBM = pl.BlockSpec(memory_space=pltpu.HBM)
SM = pl.BlockSpec(memory_space=pltpu.SMEM)


def dot_t(left, right):
    return lax.dot_general(left, right, (((1,), (1,)), ((), ())), preferred_element_type=F32)


def role(level):
    return lax.rem(lax.axis_index("pcol") + 2 * LEVELS * LR * lax.axis_size("pcol") - level * LR, lax.axis_size("pcol"))


def call(body, outs, ins, specs=None, aliases=None, scratch=(), limit=LIMIT):
    specs = specs or [VM] * len(ins)
    ins = [pltpu.with_memory_space_constraint(x, spec.memory_space) for x, spec in zip(ins, specs)]
    return pl.pallas_call(
        body,
        out_shape=[pltpu.VMEM(shape, kind) for shape, kind in outs],
        in_specs=specs,
        out_specs=[VM] * len(outs),
        input_output_aliases=aliases or {},
        scratch_shapes=scratch,
        compiler_params=pltpu.CompilerParams(vmem_limit_bytes=limit),
    )(*ins)


def row_sum(table, store, own, other, level, row, pair):
    slots = own.shape[1] - 1
    total = None
    for j in range(slots):
        at = table[level * LR + row, pair * slots + j]
        part = dot_t(store[at], (other if pair else own)[row, j])
        total = part if total is None else total + part
    return total


def update(level, table, store, pieces, own, other):
    newest = level - 1
    last = level == LEVELS - 1
    base = newest * LR // lax.axis_size("pcol") * 2 * len(pieces)

    def body(table_ref, store_ref, own_ref, other_ref, *refs):
        pieces_refs, out, sums = refs[:len(pieces)], refs[len(pieces)], refs[len(pieces) + 1:]
        place = role(newest)

        @pl.when(place < LR)
        def _():
            for j, piece in enumerate(pieces_refs):
                out[pl.ds(base + 2 * j, 2)] = piece[...]
            if not last:
                add_rows(level, place, table_ref, out, own_ref, other_ref, sums)

        if last:
            add_rows(level, place, table_ref, out, own_ref, other_ref, sums)
        else:
            @pl.when(place >= LR)
            def _():
                for to in sums:
                    to[...] = pieces_refs[0][...]

    shape = (2,) + store.shape[1:]
    sums = [((LR,) + shape, BF16)] if last else [(shape, BF16), (shape, BF16)]
    return call(body, [(store.shape, BF16), *sums], [table, store, own, other, *pieces],
                specs=[SM] + [VM] * (3 + len(pieces)), aliases={1: 0})


def add_rows(level, place, table, store, own, other, sums):
    for turn in range(LR):
        row = turn if len(sums) == 1 else lax.rem(place + turn, LR)
        for pair in range(2):
            total = row_sum(table, store, own, other, level, row, pair)
            if len(sums) == 1:
                sums[0][turn, pair] = total.astype(BF16)
            else:
                sums[turn][pair] = total.astype(sums[turn].dtype)


def early(level, newest, table, store, own, other, kind, solved):
    def body(table_ref, store_ref, own_ref, other_ref, solved_ref, *sums):
        place = role(newest)

        @pl.when(place < LR)
        def _():
            add_rows(level, place, table_ref, store_ref, own_ref, other_ref, sums)

        @pl.when(place >= LR)
        def _():
            sums[1][...] = solved_ref[...]

    shape = (2,) + store.shape[1:]
    return call(body, [(shape, kind), (shape, BF16)], [table, store, own, other, solved], specs=[SM, VM, VM, VM, VM])


def solve(level, rhs_own, rhs_other, own, other, before, terms):
    def body(ro, rp, io, ip, old, *refs):
        *terms_refs, out = refs
        place = role(level)

        @pl.when(place < LR)
        def _():
            for pair in range(2):
                r_ref, i_ref = (rp, ip) if pair else (ro, io)
                rest = r_ref[level * LR + place].astype(F32)
                for term in terms_refs:
                    rest = rest - term[pair].astype(F32)
                out[pair] = dot_t(rest.astype(BF16), i_ref[place, i_ref.shape[1] - 1]).astype(BF16)

        @pl.when(place >= LR)
        def _():
            out[...] = old[...]

    return call(body, [(before.shape, BF16)], [rhs_own, rhs_other, own, other, before, *terms])[0]


def solve_first(rhs, inverses, half):
    def body(r, i, keep, send, side, tile, sems):
        place = role(0)
        core = lax.rem(lax.axis_index("prow"), 2)
        at = lax.rem(place, LR)
        copies = [pltpu.make_async_copy(r.at[at], side, sems.at[0]), pltpu.make_async_copy(i.at[at], tile, sems.at[1])]
        for copy in copies:
            copy.start()
        for copy in copies:
            copy.wait()
        for out, part in ((keep, core), (send, 1 - core)):
            out[...] = dot_t(side[pl.ds(pl.multiple_of(part * half, half), half)], tile[...]).astype(BF16)

    size = rhs.shape[2]
    shape = ((half, size), BF16)
    return call(body, [shape, shape], [rhs, inverses], specs=[HBM] * 2,
                scratch=[pltpu.VMEM(rhs.shape[1:], BF16), pltpu.VMEM((size, size), BF16), pltpu.SemaphoreType.DMA((2,))])


def join(a, b):
    def body(x, y, out):
        out[0] = x[...]
        out[1] = y[...]

    return call(body, [((2,) + a.shape, BF16)], [a, b])[0]


def stage(level, inverses, blocks, after=()):
    slots = blocks.shape[1]
    rows = pl.ds(level * LR, LR)

    def body(i, b, *refs):
        out, sems = refs[-2:]
        copies = [pltpu.make_async_copy(b.at[rows], out.at[:, pl.ds(0, slots)], sems.at[0]),
                  pltpu.make_async_copy(i.at[rows], out.at[:, slots], sems.at[1])]
        for copy in copies:
            copy.start()
        for copy in copies:
            copy.wait()

    return call(body, [((LR, slots + 1) + blocks.shape[2:], BF16)], [inverses, blocks, *after],
                specs=[HBM] * 2 + [SM if x.dtype == jnp.int32 else VM for x in after], scratch=[pltpu.SemaphoreType.DMA((2,))])[0]


def halves(rhs, half):
    def body(r, mine, give, sems):
        core = lax.rem(lax.axis_index("prow"), 2)
        copies = []
        for k, (out, part) in enumerate(((mine, core), (give, 1 - core))):
            copies.append(pltpu.make_async_copy(r.at[:, pl.ds(pl.multiple_of(part * half, half), half)], out, sems.at[k]))
        for copy in copies:
            copy.start()
        for copy in copies:
            copy.wait()

    shape = ((rhs.shape[0], half, rhs.shape[2]), BF16)
    return call(body, [shape, shape], [rhs], specs=[HBM], scratch=[pltpu.SemaphoreType.DMA((2,))])


def zeros(shape):
    def body(out):
        out[...] = jnp.zeros(shape, BF16)

    return call(body, [(shape, BF16)], [])[0]


def to_scalars(table):
    def body(x, out):
        for i in range(table.shape[0]):
            for j in range(table.shape[1]):
                out[i, j] = x[i, j]

    return pl.pallas_call(body, out_shape=pltpu.SMEM(table.shape, jnp.int32), in_specs=[SM], out_specs=SM)(table)


def place_rows(found, col, write):
    for level, ref, away in found:
        source = jnp.bitwise_xor(col, away)
        count = lax.axis_size("pcol")
        place = lax.rem(source + 2 * LEVELS * LR * count - level * LR, count)

        @pl.when(place < LR)
        def _():
            write(level * LR + place, ref)


def pack(found, late, first):
    half, size = late[0].shape[1:]

    def body(*refs):
        sources, late_refs, out = refs[:len(found)], refs[len(found):-1], refs[-1]

        def write(row, ref):
            out[row] = ref[1]

        place_rows([(level, ref, away) for (level, _, away), ref in zip(found, sources)], lax.axis_index("pcol"), write)
        for i, ref in enumerate(late_refs):
            out[first * LR + i] = ref[1]

    return call(body, [((first * LR + len(late), half, size), BF16)], [*[x for _, x, _ in found], *late])[0]


def whole_rows(late, swapped, first):
    def body(*refs):
        late_refs, swapped_ref, outs = refs[:len(late)], refs[len(late)], refs[len(late) + 1:]
        for i, (ref, out) in enumerate(zip(late_refs, outs)):
            out[0] = ref[0]
            out[1] = swapped_ref[first * LR + i]

    return call(body, [(y.shape, BF16) for y in late], [*late, swapped])


def solve_last(rhs_own, rhs_other, own_tiles, other_tiles, parts):
    count = len(parts)

    def body(ro, rp, io, ip, *refs):
        *parts_refs, own, send, held = refs
        col = lax.axis_index("pcol")
        for k in range(count):
            held[jnp.bitwise_xor(col, k)] = parts_refs[k][...]
        for r_ref, i_ref, pair, out in ((rp, ip, 1, send), (ro, io, 0, own)):
            for row in range(LR):
                rest = r_ref[(LEVELS - 1) * LR + row].astype(F32)
                for k in range(count):
                    rest = rest - held[k, row, pair].astype(F32)
                out[row] = dot_t(rest.astype(BF16), i_ref[row, i_ref.shape[1] - 1]).astype(BF16)

    shape = ((LR,) + rhs_own.shape[1:], BF16)
    return call(body, [shape, shape], [rhs_own, rhs_other, own_tiles, other_tiles, *parts],
                scratch=[pltpu.VMEM((count,) + parts[0].shape, BF16)])


def assemble(found, late, swapped, own, last_swapped, shape, first):
    half = shape[1] // 2

    def body(*refs):
        sources, (swapped_ref, own_ref, last_ref, out) = refs[:-4], refs[-4:]
        col = lax.axis_index("pcol")
        core = lax.rem(lax.axis_index("prow"), 2)
        mine_at = pl.ds(pl.multiple_of(core * half, half), half)
        theirs_at = pl.ds(pl.multiple_of((1 - core) * half, half), half)

        def write(row, ref):
            out[row, mine_at] = ref[0]

        def write_both(row, ref):
            out[row, mine_at] = ref[0]
            out[row, theirs_at] = ref[1]

        place_rows([(level, ref, away) for (level, _, away), ref in zip(found, sources)], col, write)
        place_rows([(level, ref, away) for (level, _, away), ref in zip(late, sources[len(found):])], col, write_both)
        for row in range(first * LR):
            out[row, theirs_at] = swapped_ref[row]
        for i in range(LR):
            out[(LEVELS - 1) * LR + i, mine_at] = own_ref[i]
            out[(LEVELS - 1) * LR + i, theirs_at] = last_ref[i]

    ins = [*[x for _, x, _ in found + late], swapped, own, last_swapped]
    ins = [pltpu.with_memory_space_constraint(x, pltpu.VMEM) for x in ins]
    return pl.pallas_call(body, out_shape=jax.ShapeDtypeStruct(shape, BF16), in_specs=[VM] * len(ins), out_specs=VM,
                          compiler_params=pltpu.CompilerParams(vmem_limit_bytes=LIMIT))(*ins)


def body(rhs, blocks, inverses, columns, counts):
    rows, sides, size = rhs.shape
    slots = columns.shape[1]
    half = sides // 2
    prow_count = lax.axis_size("prow")
    pcol_count = lax.axis_size("pcol")
    groups = pcol_count // LR
    paired = groups == 2
    me = lax.axis_index("prow")

    def prow_swap(x, k):
        return lax.ppermute(x, "prow", [(i, i ^ k) for i in range(prow_count)])

    def pcol_swap(x, k):
        return lax.ppermute(x, "pcol", [(i, i ^ k) for i in range(pcol_count)])

    def between(x, first, second, turn):
        pairs = []
        for a in range(LR):
            s, d = (first * LR + a) % pcol_count, (second * LR + (a + turn) % LR) % pcol_count
            pairs += [(s, d), (d, s)]
        return lax.ppermute(x, "pcol", sorted(set(pairs)))

    def share(x):
        return [x] + [pcol_swap(x, k) for k in range(1, pcol_count)]

    keep, send = solve_first(rhs, inverses, half)
    solved = [join(keep, prow_swap(send, 1))]
    held = {1: stage(1, inverses, blocks)}
    other = {1: prow_swap(held[1], 1)}
    live = jnp.arange(slots, dtype=jnp.int32)[None, :] < counts
    coded = jnp.where(live, columns, -1)
    coded = jnp.concatenate([coded, prow_swap(coded, 1)], axis=1)
    zero_row = rows // pcol_count * prow_count
    at = coded // prow_count // pcol_count * prow_count + ((coded % prow_count) ^ me)
    table = to_scalars(jnp.where(coded < 0, zero_row, at))
    mine, give = halves(rhs, half)
    theirs = prow_swap(give, 1)

    store = zeros((zero_row + 1, half, size))
    waiting = {level: [] for level in range(LEVELS)}
    found = []
    for level in range(1, LEVELS):
        newest = level - 1
        last = level == LEVELS - 1
        y = solved[newest]
        pieces = [y]
        for k in range(2, prow_count, 2):
            pieces.append(prow_swap(y, k))
        if last:
            late = [([newest - g for g in range(groups)], y)] if paired else [([i], x) for i, x in enumerate(solved)]
            first = min(min(levels) for levels, _ in late)
            swapped = prow_swap(pack(found, [x for _, x in late], first), 1)
        if level == 1 and groups > 1:
            held[2] = stage(2, inverses, blocks, (table,))
            other[2] = prow_swap(held[2], 1)
        if level == 2 and level + groups - 1 < LEVELS:
            later = level + groups - 1
            held[later] = stage(later, inverses, blocks, (y,))
            other[later] = prow_swap(held[later], 1)
        store, *sums = update(level, table, store, pieces, held[level], other[level])
        if last:
            parts = share(sums[0])
            rows_late = whole_rows([x for _, x in late], swapped, first)
            spread = [(i, copy, k) for (levels, _), x in zip(late, rows_late)
                      for k, copy in enumerate(share(x)) for i in levels]
            own, send = solve_last(mine, theirs, held[level], other[level], parts)
            return assemble(found, spread, swapped, own, prow_swap(send, 1), rhs.shape, first)
        terms = [between(sums[0], newest, level, 0)]
        terms.append(between(sums[1], newest, level, 1))
        reach = level + groups
        for later in [reach] if level > 1 else range(3, reach):
            if later < LEVELS:
                held[later] = stage(later, inverses, blocks, sums)
                other[later] = prow_swap(held[later], 1)
        traded = None
        for ahead in range(1, groups):
            later = level + ahead
            if later >= LEVELS - 1:
                continue
            own_pair = ahead == groups - 1
            a, b = early(later, newest, table, store, held[later], other[later], F32 if own_pair else BF16, y)
            if paired:
                traded = pcol_swap(b, 1)
                waiting[later] += [a, traded]
            elif own_pair:
                waiting[later] += [a, between(b, newest, newest, 1)]
            else:
                waiting[later] += [between(a, newest, later, 0), between(b, newest, later, 1)]
        if paired and level > 1:
            if traded is None:
                traded = pcol_swap(y, 1)
            found += [(level - 2, y, 0), (level - 2, traded, 1)]
            found += [(level - 2, terms[0], 2), (level - 2, terms[1], 3)]
        solved.append(solve(level, mine, theirs, held[level], other[level], y, terms + waiting[level]))


def solution(mesh):
    placed = (
        P("prow", None, None),
        P("prow", "pcol", None, None),
        P("prow", None, None),
        P("prow", "pcol"),
        P("prow", "pcol"),
    )
    return jax.shard_map(
        body, mesh=mesh, in_specs=placed, out_specs=P("prow", None, None), check_vma=False
    )
```
